32 devices in a mesh: occ: 2 (over x), vir: 4 (over z), aux: 4 (over y, core).
Axes of the slice: x: 2, y: 2, z: 4, core: 2. Of those that a mesh axis runs over, the one named last changes fastest.
Arguments:
- amplitudes: bfloat16 [16, 1024, 1024], P('occ', 'vir'), may hold values from -6 to 6
- pair_mask: int32 [16, 8, 8], P('occ', 'vir'), may hold values 0 or 1
- left_factor: bfloat16 [32, 1024, 4096], P(None, 'vir', 'aux'), may hold values from -0.0390625 to 0.0390625
- left_mask: int32 [8, 32], P('vir', 'aux'), may hold values 0 or 1
- right_factor: bfloat16 [1024, 4, 4096], P(('occ', 'vir'), None, 'aux'), may hold values from -0.0390625 to 0.0390625
- right_mask: int32 [8, 32], P(None, 'aux'), may hold values 0 or 1
- residual_in: float32 [16, 4, 32], P('occ'), may hold values from -6 to 6
Outputs:
- updated: float32 [16, 4, 32], P('occ')
The draws below stay inside these ranges and needn't reach their ends.
All inputs are finite; a program needn't handle non-finite values. No bound on the sum of `pair_mask` or of `left_mask` or of `right_mask` on one device may be relied on, other than what follows from the above.
Results may differ from the reference program's by a relative error of at most 0.0003.
Values may be sent and summed in bfloat16 or wider, within the bound.
No kernel may reach another device: no remote copies, remote signals or barrier semaphores. Data moves between devices by JAX's collectives and lax.ppermute only.
A program may use at most 128 MiB of HBM per device.

```python
import jax
import jax.numpy as jnp
from jax import lax

V = 1024
NAUX = 4096
TILE = 128
AW = 32
BW = 4
PAIRS = 16
NVT = 8
NQT = 32


def set_ends(entries, own_key, smallest, top_value):
    dims = entries.shape
    place = [jax.random.randint(jax.random.fold_in(own_key, axis), (), 0, dims[axis]) for axis in range(len(dims))]
    entries = entries.at[tuple(place)].set(smallest)
    longest = dims.index(max(dims))
    place[longest] = (place[longest] + 1) % dims[longest]
    return entries.at[tuple(place)].set(top_value)


def block_levels(rng, dims, cuts, low, high):
    def one(dim, parts):
        draws = jax.random.uniform(jax.random.fold_in(jax.random.fold_in(rng, 6), dim), (parts,), jnp.float32, low / len(cuts), high / len(cuts))
        return jnp.repeat(jnp.exp(draws), dims[dim] // parts).reshape((-1,) + (1,) * (len(dims) - dim - 1))

    level = one(*cuts[0])
    for cut in cuts[1:]:
        level = level * one(*cut)
    return level


def scatter_about(rng, shape, spread, bound, split=(), kind=jnp.bfloat16):
    drawn = spread * jax.random.normal(rng, shape, jnp.float32)
    if split:
        drawn = drawn * block_levels(rng, shape, split, -0.22, 0.18)
    return jnp.clip(drawn, -bound, bound).astype(kind)


def setup_inputs(seed: int = 0) -> dict:
    key_list = jax.random.split(jax.random.key(seed), 8)
    return {
        "amplitudes": scatter_about(key_list[0], (PAIRS, V, V), 1.0, 6.0, ((0, 2), (1, 4))),
        "pair_mask": set_ends((jax.random.randint(key_list[1], (PAIRS, NVT, NVT), 0, 4) < 3).astype(jnp.int32), jax.random.fold_in(key_list[1], 1), 0, 1),
        "left_factor": scatter_about(key_list[2], (AW, V, NAUX), (V * max(2, NAUX // 150)) ** -0.5, 0.0390625, ((1, 4), (2, 4))),
        "left_mask": set_ends((jax.random.randint(key_list[3], (NVT, NQT), 0, 2) < 1).astype(jnp.int32), jax.random.fold_in(key_list[3], 1), 0, 1),
        "right_factor": scatter_about(key_list[4], (V, BW, NAUX), (V * max(2, NAUX // 150)) ** -0.5, 0.0390625, ((0, 8), (2, 4))),
        "right_mask": set_ends((jax.random.randint(key_list[5], (NVT, NQT), 0, 2) < 1).astype(jnp.int32), jax.random.fold_in(key_list[5], 1), 0, 1),
        "residual_in": scatter_about(key_list[6], (PAIRS, BW, AW), 1.0, 6.0, ((0, 2),), jnp.float32),
    }


def expand_tiles(mask, width):
    grown = jnp.repeat(jnp.repeat(mask, width, axis=-2), width, axis=-1)
    return grown.astype(jnp.float32)


def reference(amplitudes, pair_mask, left_factor, left_mask, right_factor, right_mask, residual_in):
    left = left_factor.astype(jnp.float32) * expand_tiles(left_mask, TILE)[None, :, :]
    right = right_factor.astype(jnp.float32) * expand_tiles(right_mask, TILE)[:, None, :]
    right_flat = right.reshape(V, BW * NAUX)

    def one_pair(pieces):
        amp, msk = pieces
        tau = amp.astype(jnp.float32) * expand_tiles(msk, TILE)
        inner = jnp.dot(tau, right_flat, precision=lax.Precision.HIGHEST, preferred_element_type=jnp.float32)
        inner = inner.reshape(V, BW, NAUX)
        return jnp.einsum("cbq,acq->ba", inner, left, precision=lax.Precision.HIGHEST)

    ladder = lax.map(one_pair, (amplitudes, pair_mask))
    return residual_in + ladder
```

```python
import functools

import jax
import jax.numpy as jnp
from jax import lax
from jax.experimental import pallas as pl
from jax.experimental.pallas import tpu as pltpu
from jax.sharding import PartitionSpec as P

TILE = 128


def shift(x, axis, size, step):
    return lax.ppermute(x, axis, [((i + step) % size, i) for i in range(size)])


def ladder_kernel(mask_ref, *refs, n_tau, first_tile, col_block, block_b, pairs):
    tau_refs = refs[:n_tau]
    right_ref, left_ref, out_ref = refs[n_tau:]
    tile_q = pl.program_id(0)
    step_c = pl.program_id(1)

    @pl.when(jnp.logical_and(tile_q == 0, step_c == 0))
    def _():
        out_ref[...] = jnp.zeros_like(out_ref)

    col_tile = step_c * col_block // TILE

    @pl.when(mask_ref[col_tile, first_tile + tile_q] != 0)
    def _():
        right = right_ref[0]
        inner = [
            jnp.dot(t[...], right, preferred_element_type=jnp.float32) for t in tau_refs
        ]
        columns = []
        for c in range(col_block):
            rows = slice(c * pairs, (c + 1) * pairs)
            columns.append(
                jnp.concatenate(
                    [
                        part[rows, b * TILE : (b + 1) * TILE]
                        for b in range(block_b)
                        for part in inner
                    ],
                    axis=0,
                )
            )
        wide = jnp.concatenate(columns, axis=1)
        high = wide.astype(jnp.bfloat16)
        low = (wide - high.astype(jnp.float32)).astype(jnp.bfloat16)
        left = jnp.concatenate([left_ref[c] for c in range(col_block)], axis=1)
        dims = (((1,), (1,)), ((), ()))
        both = jnp.concatenate([high, low], axis=0)
        got = lax.dot_general(both, left, dims, preferred_element_type=jnp.float32)
        n = wide.shape[0]
        out_ref[...] += got[:n] + got[n:]


def ladder_chunk(left_mask, taus, right, left, first_tile, block_b, pairs):
    n_tiles, depth, width = right.shape
    cols, block_a, _ = left.shape
    col_block = min(64, cols)
    n_tau = len(taus)
    kernel = functools.partial(
        ladder_kernel,
        n_tau=n_tau,
        first_tile=first_tile,
        col_block=col_block,
        block_b=block_b,
        pairs=pairs,
    )
    return pl.pallas_call(
        kernel,
        out_shape=jax.ShapeDtypeStruct((block_b * n_tau * pairs, block_a), jnp.float32),
        grid_spec=pltpu.PrefetchScalarGridSpec(
            num_scalar_prefetch=1,
            grid=(n_tiles, cols // col_block),
            in_specs=[
                pl.BlockSpec((col_block * pairs, depth), lambda q, c, m: (c, 0))
                for _ in range(n_tau)
            ]
            + [
                pl.BlockSpec((1, depth, width), lambda q, c, m: (q, 0, 0)),
                pl.BlockSpec(
                    (col_block, block_a, TILE), lambda q, c, m: (c, 0, first_tile + q)
                ),
            ],
            out_specs=pl.BlockSpec((block_b * n_tau * pairs, block_a), lambda q, c, m: (0, 0)),
        ),
        compiler_params=pltpu.CompilerParams(
            dimension_semantics=("arbitrary", "arbitrary"), vmem_limit_bytes=56 * 1024 * 1024
        ),
        name="ladder_chunk",
    )(left_mask, *taus, right, left)


def local(
    amplitudes,
    pair_mask,
    left_factor,
    left_mask,
    right_factor,
    right_mask,
    residual_in,
    *,
    n_occ,
    n_vir,
    n_aux,
    n_chunks,
):
    pairs, cols, virt_all = amplitudes.shape
    rows, block_b, aux_here = right_factor.shape
    block_a = left_factor.shape[0]
    tiles_all, aux_tiles = right_mask.shape
    occ = lax.axis_index("occ")
    vir = lax.axis_index("vir")

    row_tiles = ((occ * n_vir + vir) * rows + jnp.arange(rows, dtype=jnp.int32)) // TILE
    onehot = row_tiles[:, None] == jnp.arange(tiles_all, dtype=jnp.int32)[None, :]
    row_mask = jnp.sum(jnp.where(onehot[:, :, None], right_mask[None], 0), axis=1)
    right = right_factor.reshape(rows, block_b, aux_tiles, TILE).transpose(2, 0, 1, 3)
    right = right * row_mask.T[:, :, None, None].astype(jnp.bfloat16)
    right = right.reshape(aux_tiles, rows, block_b * TILE)

    per = aux_tiles // n_chunks
    chunks = []
    for k in range(n_chunks):
        own = right[k * per : (k + 1) * per]
        up = own
        down = own
        got = {0: own}
        for j in range(1, (n_vir - 1) // 2 + 1):
            up = shift(up, "vir", n_vir, 1)
            down = shift(down, "vir", n_vir, -1)
            got[j] = up
            got[n_vir - j] = down
        if n_vir % 2 == 0:
            half = per // 2
            first = shift(up[:half], "vir", n_vir, 1)
            second = shift(down[half:], "vir", n_vir, -1)
            got[n_vir // 2] = jnp.concatenate([first, second], axis=0)
        chunks.append(jnp.concatenate([got[j] for j in range(n_vir)], axis=1))

    depth = virt_all // n_occ
    tau_mask = jnp.repeat(jnp.repeat(pair_mask, TILE, axis=1), TILE, axis=2)
    tau = amplitudes * tau_mask.astype(jnp.bfloat16)

    def tau_for(o):
        part = lax.dynamic_slice_in_dim(tau, o * depth, depth, axis=2)
        part = jnp.concatenate([part, part], axis=2)
        part = lax.dynamic_slice_in_dim(part, vir * rows, depth, axis=2)
        return part.transpose(1, 0, 2).reshape(cols * pairs, depth)

    taus = [tau_for(occ)]
    for s in range(1, n_occ):
        taus.append(shift(tau_for((occ - s) % n_occ), "occ", n_occ, s))

    left = left_factor.transpose(1, 0, 2)

    total = None
    for k in range(n_chunks):
        part = ladder_chunk(left_mask, taus, chunks[k], left, k * per, block_b, pairs)
        total = part if total is None else total + part

    total = total.reshape(block_b, n_occ, pairs, block_a)
    grid = [(o, q) for o in range(n_occ) for q in range(n_aux)]
    mine = total[:, 0]
    for s in range(n_occ):
        for t in range(n_aux):
            if s == 0 and t == 0:
                continue
            perm = [
                (o * n_aux + q, ((o + s) % n_occ) * n_aux + (q + t) % n_aux) for o, q in grid
            ]
            mine = mine + lax.ppermute(total[:, s], ("occ", "aux"), perm)
    others = [shift(mine, "vir", n_vir, j) for j in range(1, n_vir)]
    ladder = mine
    for other in others:
        ladder = ladder + other
    return residual_in + ladder.transpose(1, 0, 2)


def solution(mesh):
    body = functools.partial(
        local,
        n_occ=mesh.shape["occ"],
        n_vir=mesh.shape["vir"],
        n_aux=mesh.shape["aux"],
        n_chunks=4,
    )
    return jax.shard_map(
        body,
        mesh=mesh,
        in_specs=(
            P("occ", "vir", None),
            P("occ", "vir", None),
            P(None, "vir", "aux"),
            P("vir", "aux"),
            P(("occ", "vir"), None, "aux"),
            P(None, "aux"),
            P("occ", None, None),
        ),
        out_specs=P("occ", None, None),
        check_vma=False,
    )
```

```python
import functools

import jax
import jax.numpy as jnp
from jax import lax
from jax.experimental import pallas as pl
from jax.experimental.pallas import tpu as pltpu
from jax.sharding import PartitionSpec as P

TILE = 128


def shift(x, axis, size, step):
    return lax.ppermute(x, axis, [((i + step) % size, i) for i in range(size)])


def ladder_kernel(mask_ref, *refs, n_tau, first_tile, col_block, block_b, pairs):
    tau_refs = refs[:n_tau]
    right_ref, left_ref, out_ref = refs[n_tau:]
    step_c = pl.program_id(0)
    tile_q = pl.program_id(1)

    @pl.when(jnp.logical_and(tile_q == 0, step_c == 0))
    def _():
        out_ref[...] = jnp.zeros_like(out_ref)

    col_tile = step_c * col_block // TILE

    @pl.when(mask_ref[col_tile, first_tile + tile_q] != 0)
    def _():
        right = right_ref[tile_q]
        tau = jnp.concatenate([t[...] for t in tau_refs], axis=0)
        inner = jnp.dot(tau, right, preferred_element_type=jnp.float32)
        size = col_block * pairs
        inner = [inner[s * size : (s + 1) * size] for s in range(n_tau)]
        columns = []
        for c in range(col_block):
            rows = slice(c * pairs, (c + 1) * pairs)
            columns.append(
                jnp.concatenate(
                    [
                        part[rows, b * TILE : (b + 1) * TILE]
                        for b in range(block_b)
                        for part in inner
                    ],
                    axis=0,
                )
            )
        wide = jnp.concatenate(columns, axis=1)
        high = wide.astype(jnp.bfloat16)
        low = (wide - high.astype(jnp.float32)).astype(jnp.bfloat16)
        left = jnp.concatenate([left_ref[c] for c in range(col_block)], axis=1)
        dims = (((1,), (1,)), ((), ()))
        both = jnp.concatenate([high, low], axis=0)
        got = lax.dot_general(both, left, dims, preferred_element_type=jnp.float32)
        n = wide.shape[0]
        out_ref[...] += got[:n] + got[n:]


def ladder_chunk(left_mask, taus, right, left, first_tile, block_b, pairs):
    n_tiles, depth, width = right.shape
    cols, block_a, _ = left.shape
    col_block = min(128, cols)
    n_tau = len(taus)
    kernel = functools.partial(
        ladder_kernel,
        n_tau=n_tau,
        first_tile=first_tile,
        col_block=col_block,
        block_b=block_b,
        pairs=pairs,
    )
    return pl.pallas_call(
        kernel,
        out_shape=jax.ShapeDtypeStruct((block_b * n_tau * pairs, block_a), jnp.float32),
        grid_spec=pltpu.PrefetchScalarGridSpec(
            num_scalar_prefetch=1,
            grid=(cols // col_block, n_tiles),
            in_specs=[
                pl.BlockSpec((col_block * pairs, depth), lambda c, q, m: (c, 0))
                for _ in range(n_tau)
            ]
            + [
                pl.BlockSpec((n_tiles, depth, width), lambda c, q, m: (0, 0, 0)),
                pl.BlockSpec(
                    (col_block, block_a, TILE), lambda c, q, m: (c, 0, first_tile + q)
                ),
            ],
            out_specs=pl.BlockSpec((block_b * n_tau * pairs, block_a), lambda c, q, m: (0, 0)),
        ),
        compiler_params=pltpu.CompilerParams(
            dimension_semantics=("arbitrary", "arbitrary"), vmem_limit_bytes=56 * 1024 * 1024
        ),
        cost_estimate=pl.CostEstimate(
            flops=2 * n_tau * pairs * cols * depth * width * n_tiles,
            bytes_accessed=2 * (n_tau * pairs * cols * depth + right.size),
            transcendentals=0,
        ),
        name="ladder_chunk",
    )(left_mask, *taus, right, left)


def local(
    amplitudes,
    pair_mask,
    left_factor,
    left_mask,
    right_factor,
    right_mask,
    residual_in,
    *,
    n_occ,
    n_vir,
    n_aux,
    n_chunks,
):
    pairs, cols, virt_all = amplitudes.shape
    rows, block_b, aux_here = right_factor.shape
    block_a = left_factor.shape[0]
    tiles_all, aux_tiles = right_mask.shape
    occ = lax.axis_index("occ")
    vir = lax.axis_index("vir")

    row_tiles = ((occ * n_vir + vir) * rows + jnp.arange(rows, dtype=jnp.int32)) // TILE
    onehot = row_tiles[:, None] == jnp.arange(tiles_all, dtype=jnp.int32)[None, :]
    row_mask = jnp.sum(jnp.where(onehot[:, :, None], right_mask[None], 0), axis=1)
    right = right_factor.reshape(rows, block_b, aux_tiles, TILE).transpose(2, 0, 1, 3)
    right = right * row_mask.T[:, :, None, None].astype(jnp.bfloat16)
    right = right.reshape(aux_tiles, rows, block_b * TILE)

    right, amplitudes, left_factor = lax.optimization_barrier((right, amplitudes, left_factor))

    per = aux_tiles // n_chunks
    rings = []
    for k in range(n_chunks):
        own = right[k * per : (k + 1) * per]
        up = own
        down = own
        got = {0: own}
        for j in range(1, (n_vir - 1) // 2 + 1):
            up = shift(up, "vir", n_vir, 1)
            down = shift(down, "vir", n_vir, -1)
            got[j] = up
            got[n_vir - j] = down
        rings.append((got, up, down))

    chunks = []
    left = left_factor.transpose(1, 0, 2)
    for k in range(n_chunks):
        got, up, down = rings[k]
        if n_vir % 2 == 0:
            half = per // 2
            first, second = up[:half], down[half:]
            if k == 0:
                first, second, left = lax.optimization_barrier((first, second, left))
            first = shift(first, "vir", n_vir, 1)
            second = shift(second, "vir", n_vir, -1)
            got[n_vir // 2] = (first, second)
        chunks.append(got)

    depth = virt_all // n_occ
    tau_mask = jnp.repeat(pair_mask.astype(jnp.bfloat16), TILE, axis=2)[:, :, None, :]
    tau = amplitudes.reshape(pairs, cols // TILE, TILE, virt_all) * tau_mask
    tau = tau.reshape(amplitudes.shape)

    def tau_for(o):
        part = lax.dynamic_slice_in_dim(tau, o * depth, depth, axis=2)
        part = jnp.concatenate([part, part], axis=2)
        part = lax.dynamic_slice_in_dim(part, vir * rows, depth, axis=2)
        return part.transpose(1, 0, 2).reshape(cols * pairs, depth)

    taus = [tau_for(occ)]
    for s in range(1, n_occ):
        taus.append(shift(tau_for((occ - s) % n_occ), "occ", n_occ, s))

    total = None
    for k in range(n_chunks):
        got = chunks[k]
        if n_vir % 2 == 0:
            first, second = got[n_vir // 2]
            if total is not None:
                first, second, total = lax.optimization_barrier((first, second, total))
            got[n_vir // 2] = jnp.concatenate([first, second], axis=0)
        whole = jnp.concatenate([got[j] for j in range(n_vir)], axis=1)
        part = ladder_chunk(left_mask, taus, whole, left, k * per, block_b, pairs)
        total = part if total is None else total + part

    total = total.reshape(block_b, n_occ, pairs, block_a)
    grid = [(o, q) for o in range(n_occ) for q in range(n_aux)]
    mine = total[:, 0]
    for s in range(n_occ):
        for t in range(n_aux):
            if s == 0 and t == 0:
                continue
            perm = [
                (o * n_aux + q, ((o + s) % n_occ) * n_aux + (q + t) % n_aux) for o, q in grid
            ]
            mine = mine + lax.ppermute(total[:, s], ("occ", "aux"), perm)
    others = [shift(mine, "vir", n_vir, j) for j in range(1, n_vir)]
    ladder = mine
    for other in others:
        ladder = ladder + other
    return residual_in + ladder.transpose(1, 0, 2)


def solution(mesh):
    body = functools.partial(
        local,
        n_occ=mesh.shape["occ"],
        n_vir=mesh.shape["vir"],
        n_aux=mesh.shape["aux"],
        n_chunks=2,
    )
    return jax.shard_map(
        body,
        mesh=mesh,
        in_specs=(
            P("occ", "vir", None),
            P("occ", "vir", None),
            P(None, "vir", "aux"),
            P("vir", "aux"),
            P(("occ", "vir"), None, "aux"),
            P(None, "aux"),
            P("occ", None, None),
        ),
        out_specs=P("occ", None, None),
        check_vma=False,
    )
```
